32 devices in a mesh: band: 8 (over y, x, core), sub: 4 (over z).
Axes of the slice: x: 2, y: 2, z: 4, core: 2. Of those that a mesh axis runs over, the one named last changes fastest.
Arguments:
- fields: bfloat16 [12, 1048576], P(None, ('band', 'sub')), may hold values from -1.5 to 6
- land_mask: int32 [1048576], P(('band', 'sub')), may hold values from 0 to 1
- intersection: bfloat16 [8192, 128, 128], P(('band', 'sub')), as said below
- send_slot: int32 [8192], P(('band', 'sub')), may hold values from 0 to 511, as said below
- target_block: int32 [8192], P(('band', 'sub')), may hold values from 0 to 15
- live_blocks: int32 [32], P(('band', 'sub')), may hold values from 192 to 256, as said below
Outputs:
- remapped: float32 [12, 65536], P(None, ('band', 'sub'))
The draws below stay inside these ranges and needn't reach their ends.
Inputs may be any that keep to these rules, and one draw needn't show every extreme that they name: `send_slot`: within one device's 256 entries the values are distinct; value // 16 is the device that owns the block's target; in each device's entries some owner is named exactly 16 times and none more. `live_blocks`: some device has all 256 slots live in every draw. `intersection`: entries are positive.
All inputs are finite; a program needn't handle non-finite values.
Results may differ from the reference program's by a relative error of at most 0.0003.
Values may be sent and summed in bfloat16 or wider, within the bound.
A program may use at most 64 MiB of HBM per device.

```python
import jax
import jax.numpy as jnp
from jax import lax

F = 12
CELL = 128
SB_DEV = 256
TB_DEV = 16
CAP = 16
SB = 8192
TB = 512
DEVICES = 32


def draw_intersection(key, part):
    first_key, second_key = jax.random.split(jax.random.fold_in(key, 11), 2)
    logs = jax.random.uniform(first_key, (SB, CELL, CELL), jnp.float32, jnp.log(0.001), jnp.log(0.02))
    offdiag = jnp.exp(logs)
    diagonal = jax.random.uniform(second_key, (SB, CELL), jnp.float32, 0.15, 0.35)
    weights = offdiag + jnp.eye(CELL, dtype=jnp.float32)[None, :, :] * diagonal[:, :, None]
    return weights.astype(jnp.bfloat16)


def draw_send_slot(key, part):
    base_key = jax.random.fold_in(key, 23)

    def device_slots(device):
        random_device_key = jax.random.fold_in(base_key, device)
        first_key, second_key, third_key = jax.random.split(random_device_key, 3)
        positions = DEVICES * CAP
        scores = jax.random.permutation(first_key, positions).astype(jnp.int32)
        chosen_owner = jax.random.randint(second_key, (), 0, DEVICES)
        places = jnp.arange(positions, dtype=jnp.int32)
        scores = jnp.where(places // CAP == chosen_owner, positions + places, scores)
        top_values, top_places = lax.top_k(scores, SB_DEV)
        ordering = jax.random.permutation(third_key, SB_DEV)
        return top_places[ordering].astype(jnp.int32)
    return jax.vmap(device_slots)(jnp.arange(DEVICES, dtype=jnp.int32)).reshape(-1)


def target_numbers(key):
    return jax.random.randint(jax.random.fold_in(key, 41), (SB,), 0, TB_DEV).astype(jnp.int32)


def draw_target_block(key, part):
    return target_numbers(key)


def draw_land_mask(key, part):
    slots = draw_send_slot(key, part)
    global_target = slots // CAP * TB_DEV + target_numbers(key)
    kinds = jax.random.randint(jax.random.fold_in(key, 43), (TB,), 0, 16).astype(jnp.int32)
    block_kind = kinds[global_target]
    first_key, second_key = jax.random.split(jax.random.fold_in(key, 47))
    block_draw = jax.random.randint(first_key, (SB,), 0, 16).astype(jnp.int32)
    cell_draw = jax.random.randint(second_key, (SB, CELL), 0, 16).astype(jnp.int32)
    coastal = (block_kind >= 1) & (block_kind < 4)
    inland = block_kind >= 4
    coastal_land = (coastal & (block_draw < 2))[:, None] & (cell_draw < 4)
    inland_land = (inland & (block_draw >= 5))[:, None] & (cell_draw < 13)
    land = (coastal_land | inland_land).astype(jnp.int32)
    return land.reshape(SB * CELL)


def draw_fields(key, part):
    first_key = jax.random.fold_in(jax.random.fold_in(key, 53), 0)
    device = (jnp.arange(SB * CELL, dtype=jnp.int32) // (SB_DEV * CELL)).astype(jnp.float32)
    position = device / max(DEVICES - 1, 1)
    level = (0.5 + 2.0 * position)[None, :]
    noise = jax.random.uniform(first_key, (F, SB * CELL), jnp.float32, -1.0, 1.0)
    return (level + noise).astype(jnp.bfloat16)


def draw_live_blocks(key, part):
    first_key, second_key = jax.random.split(jax.random.fold_in(key, 37))
    counts = jax.random.randint(first_key, (DEVICES,), 3 * SB_DEV // 4, SB_DEV + 1)
    full_device = jax.random.randint(second_key, (), 0, DEVICES)
    counts = jnp.where(jnp.arange(DEVICES) == full_device, SB_DEV, counts)
    return counts.astype(jnp.int32)


def setup_inputs(seed: int = 0) -> dict:
    streams_of = jax.random.split(jax.random.key(seed), 7)
    fields = draw_fields(jax.random.fold_in(streams_of[6], 71), 0)
    land_mask = draw_land_mask(jax.random.fold_in(streams_of[6], 71), 0)
    intersection = draw_intersection(jax.random.fold_in(streams_of[6], 71), 0)
    send_slot = draw_send_slot(jax.random.fold_in(streams_of[6], 71), 0)
    target_block = draw_target_block(jax.random.fold_in(streams_of[6], 71), 0)
    live_blocks = draw_live_blocks(jax.random.fold_in(streams_of[6], 71), 0)
    return dict(fields=fields, land_mask=land_mask, intersection=intersection, send_slot=send_slot, target_block=target_block, live_blocks=live_blocks)


def reference(fields, land_mask, intersection, send_slot, target_block, live_blocks):
    field_blocks = fields.reshape(F, DEVICES, SB_DEV, CELL).transpose(1, 2, 0, 3)
    mask_blocks = land_mask.reshape(DEVICES, SB_DEV, CELL)
    live_rows = (jnp.arange(SB_DEV, dtype=jnp.int32)[None, :] < live_blocks[:, None]).astype(jnp.int32)
    kept_mask = mask_blocks * live_rows[:, :, None]
    kept_float = kept_mask.astype(jnp.float32)
    masked = field_blocks * kept_mask[:, :, None, :].astype(jnp.bfloat16)
    totals = jnp.sum(masked.astype(jnp.float32), axis=(0, 1, 3))
    land_count = jnp.sum(kept_float)
    land_mean = totals / jnp.maximum(land_count, 1.0)
    stacked_fields = jnp.concatenate([masked, kept_mask[:, :, None, :].astype(jnp.bfloat16)], axis=2)
    weights = intersection.reshape(DEVICES, SB_DEV, CELL, CELL)
    global_target = ((send_slot.reshape(DEVICES, SB_DEV) // CAP) * TB_DEV + target_block.reshape(DEVICES, SB_DEV)).astype(jnp.int32)

    def add_device(accumulated, items):
        field_stack_part, remap_weight_part, target_part = items
        contribution_partial = jnp.einsum("myr,mrw->myw", field_stack_part.astype(jnp.float32), remap_weight_part.astype(jnp.float32))
        return accumulated.at[target_part].add(contribution_partial), None

    start_sums = jnp.zeros((TB_DEV * DEVICES, F + 1, CELL), jnp.float32)
    sums, unused = lax.scan(add_device, start_sums, (stacked_fields, weights, global_target))
    numer = sums[:, :F, :]
    fraction = sums[:, F, :]
    filled = numer + jnp.maximum(0.25 - fraction, 0.0)[:, None, :] * land_mean[None, :, None]
    remap_output = filled / jnp.maximum(fraction, 0.25)[:, None, :]
    return remap_output.transpose(1, 0, 2).reshape(F, TB_DEV * DEVICES * CELL)
```

```python
import functools
import itertools
import math

import jax
import jax.numpy as jnp
from jax import lax
from jax.experimental import pallas as pl
from jax.experimental.pallas import tpu as pltpu
from jax.sharding import PartitionSpec as P

TB_DEV = 16
GROUP = 16
TILE = 8
PIECES = TB_DEV // TILE
LEVELS = 32700.0


def in_hbm(a):
    return pltpu.with_memory_space_constraint(a, pltpu.HBM)


def split(value, size):
    if size & (size - 1) == 0:
        return value >> (size.bit_length() - 1), value & (size - 1)
    return lax.div(value, size), lax.rem(value, size)


def contribute(
    capacity, rows, owners, slot_hbm, target_hbm, live_hbm, f_hbm, m_hbm, w_hbm, acc_ref,
    f_all, m_all, w_all, fx, products, tot, top, slot_ref, target_ref, live_ref, sem, scalar_sem,
):
    field_count = f_hbm.shape[0]
    cells = w_hbm.shape[2]
    steps = f_all.shape[0]
    width = GROUP * cells

    def copies(i):
        return (
            pltpu.make_async_copy(m_hbm.at[pl.ds(i * GROUP, GROUP)], m_all.at[i], sem.at[0, i]),
            pltpu.make_async_copy(f_hbm.at[:, pl.ds(i * width, width)], f_all.at[i], sem.at[1, i]),
            pltpu.make_async_copy(w_hbm.at[pl.ds(i * GROUP, GROUP)], w_all.at[i], sem.at[2, i]),
        )

    scalars = (
        pltpu.make_async_copy(slot_hbm, slot_ref, scalar_sem.at[0]),
        pltpu.make_async_copy(target_hbm, target_ref, scalar_sem.at[1]),
        pltpu.make_async_copy(live_hbm, live_ref, scalar_sem.at[2]),
    )
    for copy in scalars:
        copy.start()
    for i in range(steps):
        for copy in copies(i):
            copy.start()

    part = rows * PIECES

    def clear(k, carry):
        acc_ref[pl.ds(pl.multiple_of(k * part, 8), part), :] = jnp.zeros((part, cells), jnp.float32)
        return carry

    lax.fori_loop(0, owners, clear, 0)
    tot[...] = jnp.zeros_like(tot)
    top[...] = jnp.zeros_like(top)
    products[...] = jnp.zeros_like(products)
    extra = lax.broadcasted_iota(jnp.int32, (fx.shape[0] - field_count, fx.shape[1]), 0)
    fx[field_count:, :] = jnp.where(extra == 0, 1.0, 0.0)
    for copy in scalars:
        copy.wait()
    live = live_ref[0]
    place = lax.broadcasted_iota(jnp.int32, (GROUP, cells), 0)

    def accumulate(first, half):
        for j in range(GROUP):
            b = first + j
            owner, _ = split(slot_ref[b], capacity)
            piece, target = split(target_ref[b], TILE)
            row = (owner * PIECES + piece) * rows + target * (field_count + 1)
            acc_ref[pl.ds(row, 16), :] += products[half, j * 16 : (j + 1) * 16, :]

    def step(i, carry):
        for copy in copies(i):
            copy.wait()
        fx[:field_count, :] = f_all[i].astype(jnp.float32)
        keep = jnp.where(i * GROUP + place < live, m_all[i], 0).astype(jnp.float32)
        total = tot[...]
        most = top[...]
        now = i & 1
        for j in range(GROUP):
            x = fx[:, j * cells : (j + 1) * cells] * keep[j : j + 1, :]
            total = total + x
            most = jnp.maximum(most, jnp.abs(x))
            products[now, j * 16 : (j + 1) * 16, :] = jnp.dot(
                x.astype(jnp.bfloat16), w_all[i, j], preferred_element_type=jnp.float32
            )
        accumulate(jnp.maximum(i - 1, 0) * GROUP, 1 - now)
        tot[...] = total
        top[...] = most
        return carry

    lax.fori_loop(0, steps, step, 0)
    accumulate((steps - 1) * GROUP, (steps - 1) & 1)
    total = tot[...]
    most = top[...]
    low = jnp.sum(total[:TILE], axis=1, keepdims=True)
    high = jnp.sum(total[TILE:], axis=1, keepdims=True)
    lane = lax.broadcasted_iota(jnp.int32, (TILE, cells), 1)
    row = lax.broadcasted_iota(jnp.int32, most.shape, 0)
    largest = jnp.max(jnp.where(row < field_count, most, 0.0))
    packed = jnp.where(lane == 0, low, jnp.where(lane == 1, high, largest))
    for chunk in range(owners * PIECES):
        start = (chunk + 1) * rows - TILE
        acc_ref[start : start + TILE, :] = packed


def exchange(sizes, orders, field_count, acc_ref, out_ref, *scratch):
    ny, nx, nz = sizes["y"], sizes["x"], sizes["z"]
    band, z = lax.axis_index("band"), lax.axis_index("sub")
    core = lax.rem(band, 2)
    x = lax.rem(band // 2, nx)
    y = band // (2 * nx)
    coords = {"y": y, "x": x, "z": z}

    def device(**moved):
        at = dict(coords, core=core)
        at.update(moved)
        return {"band": (at["y"] * nx + at["x"]) * 2 + at["core"], "sub": at["z"]}

    partners = [device(core=1 - core)]
    for name, size in sizes.items():
        for k in range(1, size):
            partners.append(device(**{name: lax.rem(coords[name] + k, size)}))
    barrier = pltpu.get_barrier_semaphore()
    for partner in partners:
        pl.semaphore_signal(barrier, inc=1, device_id=partner, device_id_type=pl.DeviceIdType.MESH)
    pl.semaphore_wait(barrier, len(partners))

    send_sem, recv_sem = scratch[-2:]
    buffers = iter(scratch[:-2])
    cells = acc_ref.shape[-1]
    lane = lax.broadcasted_iota(jnp.int32, (TILE, cells), 1)
    packed_rows = field_count * TILE
    counter = [0]
    started = []

    def send(src, dst, partner):
        k = counter[0]
        counter[0] += 1
        copy = pltpu.make_async_remote_copy(
            src_ref=src,
            dst_ref=dst,
            send_sem=send_sem.at[k],
            recv_sem=recv_sem.at[k],
            device_id=partner,
            device_id_type=pl.DeviceIdType.MESH,
        )
        copy.start()
        started.append(copy)
        return copy

    def merge(a, b):
        return jnp.where(lane < 2, a + b, jnp.maximum(a, b))

    def encode(sums, at, gain, codes, heads, to):
        fraction = sums[(*at, slice(packed_rows, packed_rows + TILE))]
        gain = jnp.where(fraction > 0.0, 1.0 / fraction, 0.0) * gain
        for f in range(0, field_count, 2):
            first = sums[(*at, slice(f * TILE, (f + 1) * TILE))] * gain
            second = sums[(*at, slice((f + 1) * TILE, (f + 2) * TILE))] * gain
            pair = jnp.concatenate([first, second], axis=0)
            code = jnp.round(pair).astype(jnp.int32).astype(jnp.int16)
            codes[(*to, slice(f * TILE, (f + 2) * TILE))] = code
        heads[to] = fraction

    def decode(codes, heads, at, gain):
        fraction = heads[at]
        gain = fraction * gain
        tiles = []
        for f in range(0, field_count, 2):
            code = codes[(*at, slice(f * TILE, (f + 2) * TILE))]
            pair = code.astype(jnp.int32).astype(jnp.float32)
            tiles += [pair[:TILE] * gain, pair[TILE:] * gain]
        return tiles + [fraction]

    class Piece:
        pass

    pieces = []
    for p, order in enumerate(orders):
        piece = Piece()
        piece.order, piece.left = order, ["y", "x", "z"]
        piece.landed, piece.sums = next(buffers), next(buffers)
        piece.steps = [[next(buffers) for _ in range(7)] for _ in order]
        src = acc_ref.at[:, :, 1 - core, :, p]
        piece.pending = [send(src, piece.landed, device(core=1 - core))]
        pieces.append(piece)

    def launch(piece, phase):
        name = piece.order[phase]
        axis = piece.left.index(name)
        out_codes, out_heads, out_extra, in_codes, in_heads, in_extra, _ = piece.steps[phase]
        out_extra[...] = piece.extra
        largest = piece.extra[:, 2:3]
        gain = jnp.where(largest > 0.0, LEVELS / jnp.maximum(largest, 1e-30), 0.0)
        rest = [sizes[d] for d in piece.left if d != name]
        piece.pending = []
        for k in range(1, sizes[name]):
            peer = lax.rem(coords[name] + k, sizes[name])
            for at in itertools.product(*[range(n) for n in rest]):
                encode(piece.sums, (*at[:axis], peer, *at[axis:]), gain, out_codes, out_heads, (k - 1, *at))
            to = device(**{name: peer})
            piece.pending.append(
                (
                    send(out_codes.at[k - 1], in_codes.at[k - 1], to),
                    send(out_heads.at[k - 1], in_heads.at[k - 1], to),
                    send(out_extra, in_extra.at[k - 1], to),
                )
            )

    def collect(piece, phase):
        name = piece.order[phase]
        axis = piece.left.index(name)
        _, _, _, in_codes, in_heads, in_extra, after = piece.steps[phase]
        rest = [sizes[d] for d in piece.left if d != name]
        for copies in piece.pending:
            for copy in copies:
                copy.wait_recv()
        extras = [in_extra[k - 1] for k in range(1, sizes[name])]
        piece.extra = functools.reduce(merge, extras, piece.extra)
        gains = [extra[:, 2:3] * (1.0 / LEVELS) for extra in extras]
        for at in itertools.product(*[range(n) for n in rest]):
            own = (*at[:axis], coords[name], *at[axis:])
            tiles = [
                piece.sums[(*own, slice(f * TILE, (f + 1) * TILE))] for f in range(field_count + 1)
            ]
            for k in range(1, sizes[name]):
                more = decode(in_codes, in_heads, (k - 1, *at), gains[k - 1])
                tiles = [a + b for a, b in zip(tiles, more)]
            for f, tile in enumerate(tiles):
                after[(*at, slice(f * TILE, (f + 1) * TILE))] = tile
        piece.left.remove(name)
        piece.sums = after

    for p, piece in enumerate(pieces):
        piece.pending[0].wait_recv()
        for yi, xi, zi in itertools.product(range(ny), range(nx), range(nz)):
            for f in range(field_count + 1):
                strided = pl.ds(f, TILE, stride=field_count + 1)
                tile = acc_ref[yi, xi, core, zi, p, strided, :] + piece.landed[yi, xi, zi, strided, :]
                piece.sums[yi, xi, zi, f * TILE : (f + 1) * TILE, :] = tile
        extra = slice(packed_rows + TILE, packed_rows + 2 * TILE)
        piece.extra = merge(acc_ref[0, 0, core, 0, p, extra, :], piece.landed[0, 0, 0, extra, :])
        launch(piece, 0)
    for phase in range(3):
        for piece in pieces:
            collect(piece, phase)
            if phase < 2:
                launch(piece, phase + 1)

    totals = pieces[0].extra
    row, column = field_count % TILE, field_count // TILE
    count = jnp.maximum(totals[row : row + 1, column : column + 1], 1.0)
    means = totals / count
    for p, piece in enumerate(pieces):
        fraction = piece.sums[packed_rows : packed_rows + TILE, :]
        short = jnp.maximum(0.25 - fraction, 0.0)
        least = jnp.maximum(fraction, 0.25)
        for f in range(field_count):
            row, column = f % TILE, f // TILE
            mean = means[row : row + 1, column : column + 1]
            numer = piece.sums[f * TILE : (f + 1) * TILE, :]
            out_ref[f, p * TILE : (p + 1) * TILE, :] = (numer + short * mean) / least
    for copy in started:
        copy.wait_send()


def body(sizes, fields, land_mask, intersection, send_slot, target_block, live_blocks):
    block_count, cells = intersection.shape[0], intersection.shape[1]
    field_count = fields.shape[0]
    nx, ny, nz = sizes["x"], sizes["y"], sizes["z"]
    owners = ny * nx * 2 * nz
    capacity = max(2, 2 * block_count // owners)
    rows = (field_count + 2) * TILE
    steps = block_count // GROUP
    acc = pl.pallas_call(
        functools.partial(contribute, capacity, rows, owners),
        in_specs=[pl.BlockSpec(memory_space=pl.ANY)] * 6,
        out_specs=pl.BlockSpec(memory_space=pltpu.VMEM),
        out_shape=jax.ShapeDtypeStruct((owners * PIECES * rows, cells), jnp.float32),
        scratch_shapes=[
            pltpu.VMEM((steps, field_count, GROUP * cells), jnp.bfloat16),
            pltpu.VMEM((steps, GROUP, cells), jnp.int32),
            pltpu.VMEM((steps, GROUP, cells, cells), jnp.bfloat16),
            pltpu.VMEM((16, GROUP * cells), jnp.float32),
            pltpu.VMEM((2, GROUP * 16, cells), jnp.float32),
            pltpu.VMEM((16, cells), jnp.float32),
            pltpu.VMEM((16, cells), jnp.float32),
            pltpu.SMEM(send_slot.shape, jnp.int32),
            pltpu.SMEM(target_block.shape, jnp.int32),
            pltpu.SMEM(live_blocks.shape, jnp.int32),
            pltpu.SemaphoreType.DMA((3, steps)),
            pltpu.SemaphoreType.DMA((3,)),
        ],
        compiler_params=pltpu.CompilerParams(
            vmem_limit_bytes=40 * 2**20
        ),
    )(
        in_hbm(send_slot),
        in_hbm(target_block),
        live_blocks,
        in_hbm(fields),
        in_hbm(land_mask.reshape(block_count, cells)),
        in_hbm(intersection),
    )
    acc = acc.reshape(ny, nx, 2, nz, PIECES, rows, cells)

    orders = (("x", "y", "z"), ("y", "z", "x"))
    scratch = []
    copies = 0
    for order in orders:
        left = ["y", "x", "z"]
        shape = [sizes[d] for d in left]
        scratch.append(pltpu.VMEM((*shape, rows, cells), jnp.float32))
        scratch.append(pltpu.VMEM((*shape, rows - TILE, cells), jnp.float32))
        copies += 1
        for name in order:
            del shape[left.index(name)]
            left.remove(name)
            sent = (sizes[name] - 1, *shape)
            codes = pltpu.VMEM((*sent, field_count * TILE, cells), jnp.int16)
            heads = pltpu.VMEM((*sent, TILE, cells), jnp.float32)
            scratch += [codes, heads, pltpu.VMEM((TILE, cells), jnp.float32)]
            scratch += [codes, heads, pltpu.VMEM((sizes[name] - 1, TILE, cells), jnp.float32)]
            scratch.append(pltpu.VMEM((*shape, rows - TILE, cells), jnp.float32))
            copies += 3 * (sizes[name] - 1)
    scratch += [pltpu.SemaphoreType.DMA((copies,))] * 2
    remapped = pl.pallas_call(
        functools.partial(exchange, sizes, orders, field_count),
        in_specs=[pl.BlockSpec(memory_space=pltpu.VMEM)],
        out_specs=pl.BlockSpec(memory_space=pltpu.VMEM),
        out_shape=jax.ShapeDtypeStruct((field_count, TB_DEV, cells), jnp.float32),
        scratch_shapes=scratch,
        compiler_params=pltpu.CompilerParams(
            collective_id=0, has_side_effects=True, vmem_limit_bytes=50 * 2**20
        ),
    )(acc)
    return remapped.reshape(field_count, TB_DEV * cells)


def solution(mesh):
    band, sub = mesh.shape["band"], mesh.shape["sub"]
    plane = band // 2
    nx = max(d for d in range(1, math.isqrt(plane) + 1) if plane % d == 0)
    sizes = {"y": plane // nx, "x": nx, "z": sub}
    return jax.shard_map(
        functools.partial(body, sizes),
        mesh=mesh,
        in_specs=(
            P(None, ("band", "sub")),
            P(("band", "sub")),
            P(("band", "sub"), None, None),
            P(("band", "sub")),
            P(("band", "sub")),
            P(("band", "sub")),
        ),
        out_specs=P(None, ("band", "sub")),
        check_vma=False,
    )
```

```python
import functools
import math

import jax
import jax.numpy as jnp
from jax import lax
from jax.experimental import pallas as pl
from jax.experimental.pallas import tpu as pltpu
from jax.sharding import PartitionSpec as P

TB_DEV = 16
GROUP = 16
TILE = 8
PIECES = TB_DEV // TILE
GAIN = 32700.0 / 6.0


def in_hbm(a):
    return pltpu.with_memory_space_constraint(a, pltpu.HBM)


def split(value, size):
    if size & (size - 1) == 0:
        return value >> (size.bit_length() - 1), value & (size - 1)
    return lax.div(value, size), lax.rem(value, size)


def contribute(
    capacity, owners, slot_hbm, target_hbm, live_hbm, f_hbm, m_hbm, w_hbm, acc_ref, tot_ref,
    f_all, m_all, w_all, fx, products, tot, slot_ref, target_ref, live_ref, sem, scalar_sem,
):
    field_count = f_hbm.shape[0]
    cells = w_hbm.shape[2]
    steps = f_all.shape[0]
    width = GROUP * cells

    def copies(i):
        return (
            pltpu.make_async_copy(m_hbm.at[pl.ds(i * GROUP, GROUP)], m_all.at[i], sem.at[0, i]),
            pltpu.make_async_copy(f_hbm.at[:, pl.ds(i * width, width)], f_all.at[i], sem.at[1, i]),
            pltpu.make_async_copy(w_hbm.at[pl.ds(i * GROUP, GROUP)], w_all.at[i], sem.at[2, i]),
        )

    scalars = (
        pltpu.make_async_copy(slot_hbm, slot_ref, scalar_sem.at[0]),
        pltpu.make_async_copy(target_hbm, target_ref, scalar_sem.at[1]),
        pltpu.make_async_copy(live_hbm, live_ref, scalar_sem.at[2]),
    )
    for copy in scalars:
        copy.start()
    for i in range(steps):
        for copy in copies(i):
            copy.start()

    stride = field_count + 1
    part = TB_DEV * stride

    def clear(k, carry):
        acc_ref[pl.ds(pl.multiple_of(k * part, 8), part), :] = jnp.zeros((part, cells), jnp.float32)
        return carry

    lax.fori_loop(0, owners, clear, 0)
    acc_ref[owners * part :, :] = jnp.zeros((TILE, cells), jnp.float32)
    tot[...] = jnp.zeros_like(tot)
    products[...] = jnp.zeros_like(products)
    extra = lax.broadcasted_iota(jnp.int32, (fx.shape[0] - field_count, fx.shape[1]), 0)
    fx[field_count:, :] = jnp.where(extra == 0, 1.0, 0.0)
    for copy in scalars:
        copy.wait()
    live = live_ref[0]
    place = lax.broadcasted_iota(jnp.int32, (GROUP, cells), 0)

    def accumulate(first, half):
        for j in range(GROUP):
            b = first + j
            owner, _ = split(slot_ref[b], capacity)
            row = (owner * TB_DEV + target_ref[b]) * stride
            acc_ref[pl.ds(row, 16), :] += products[half, j * 16 : (j + 1) * 16, :]

    def step(i, carry):
        for copy in copies(i):
            copy.wait()
        accumulate(jnp.maximum(i - 1, 0) * GROUP, (i + 1) & 1)
        fx[:field_count, :] = f_all[i].astype(jnp.float32)
        keep = jnp.where(i * GROUP + place < live, m_all[i], 0).astype(jnp.float32)
        total = tot[...]
        now = i & 1
        for j in range(GROUP):
            x = fx[:, j * cells : (j + 1) * cells] * keep[j : j + 1, :]
            total = total + x
            products[now, j * 16 : (j + 1) * 16, :] = jnp.dot(
                x.astype(jnp.bfloat16), w_all[i, j], preferred_element_type=jnp.float32
            )
        tot[...] = total
        return carry

    lax.fori_loop(0, steps, step, 0)
    accumulate((steps - 1) * GROUP, (steps - 1) & 1)
    total = tot[...]
    low = jnp.sum(total[:TILE], axis=1, keepdims=True)
    high = jnp.sum(total[TILE:], axis=1, keepdims=True)
    lane = lax.broadcasted_iota(jnp.int32, (TILE, cells), 1)
    tot_ref[...] = jnp.where(lane == 0, low, high)


def exchange(sizes, field_count, acc_ref, tot_ref, out_ref, *scratch):
    ny, nx, nz = sizes["y"], sizes["x"], sizes["z"]
    band, z = lax.axis_index("band"), lax.axis_index("sub")
    core = lax.rem(band, 2)
    x = lax.rem(band // 2, nx)
    y = band // (2 * nx)
    stride = field_count + 1
    span = TB_DEV * stride
    cells = acc_ref.shape[-1]

    def device(y, x, core, z):
        return {"band": (y * nx + x) * 2 + core, "sub": z}

    near = [(dy, dx) for dy in range(ny) for dx in range(nx)]
    near.sort(key=lambda d: -(d[0] > 0) - (d[1] > 0))
    peers = near[:-1]

    def chip(k):
        dy, dx = near[k]
        return lax.rem(y + dy, ny), lax.rem(x + dx, nx)

    def along(j):
        if j == nz - 1:
            return z
        high = (2 * z) // nz
        down = nz - 1 - j
        down = down - (z - down + nz) // nz
        up = j + (j - z + nz) // nz
        return (1 - high) * down + high * up

    partners = [device(y, x, 1 - core, z)]
    partners += [device(*chip(k), core, z) for k in range(len(peers))]
    partners += [device(y, x, core, lax.rem(z + k, nz)) for k in range(1, nz)]
    barrier = pltpu.get_barrier_semaphore()
    for partner in partners:
        pl.semaphore_signal(barrier, inc=1, device_id=partner, device_id_type=pl.DeviceIdType.MESH)
    pl.semaphore_wait(barrier, len(partners))

    (landed, out_codes, out_heads, in_codes, in_heads, far_codes, far_heads, got_codes, got_heads,
     sums, result, chip_tot, near_tot, plane_tot, far_tot, send_sem, recv_sem) = scratch
    counter = [0]
    started = []

    def claim(count=1):
        counter[0] += count
        return counter[0] - count

    def send(src, dst, partner, slot=None):
        k = claim()
        copy = pltpu.make_async_remote_copy(
            src_ref=src,
            dst_ref=dst,
            send_sem=send_sem.at[k],
            recv_sem=recv_sem.at[k if slot is None else slot],
            device_id=partner,
            device_id_type=pl.DeviceIdType.MESH,
        )
        copy.start()
        started.append(copy)
        return copy

    def first_row(k, j, core):
        at = device(*chip(k), core, along(j))
        return pl.multiple_of((at["band"] * nz + at["sub"]) * span, 8)

    def encode(load, fraction, codes, heads, at):
        gain = jnp.where(fraction > 0.0, GAIN / fraction, 0.0)
        for f in range(0, field_count, 2):
            pair = jnp.concatenate([load(f) * gain, load(f + 1) * gain], axis=0)
            codes[(*at, slice(f * TILE, (f + 2) * TILE))] = jnp.round(pair).astype(jnp.int32).astype(jnp.int16)
        heads[at] = fraction

    def decode(codes, gain, at, f):
        pair = codes[(*at, slice(f * TILE, (f + 2) * TILE))].astype(jnp.int32).astype(jnp.float32)
        return pair[:TILE] * gain, pair[TILE:] * gain

    own = len(peers)
    partner = device(y, x, 1 - core, z)
    merges = {}
    tot_copy = send(tot_ref, chip_tot.at[0], partner)
    for j in range(nz):
        for k in range(own + 1):
            rows = pl.ds(first_row(k, j, 1 - core), span)
            merges[j, k] = send(acc_ref.at[rows], landed.at[j, k], partner)

    def merged(j, k, p):
        start = first_row(k, j, core) + p * TILE * stride

        def load(f):
            there = landed[j, k, pl.ds(p * TILE * stride + f, TILE, stride=stride), :]
            return acc_ref[pl.ds(start + f, TILE, stride=stride), :] + there

        return load

    spreads = {}
    for j in range(nz):
        for k in range(own):
            merges[j, k].wait_recv()
            for p in range(PIECES):
                load = merged(j, k, p)
                encode(load, load(field_count), out_codes, out_heads, (j, k, p))
            to = device(*chip(k), core, z)
            spreads[j, k] = (
                send(out_codes.at[j, k], in_codes.at[j, k], to),
                send(out_heads.at[j, k], in_heads.at[j, k], to),
            )
    tot_copy.wait_recv()
    chip_tot[1] = tot_ref[...] + chip_tot[0]
    near_copies = [
        send(chip_tot.at[1], near_tot.at[k], device(*chip(k), core, z)) for k in range(own)
    ]

    far_slots = claim(3 * (nz - 1))
    far_copies = []
    for j in range(nz):
        merges[j, own].wait_recv()
        for k in range(own):
            for copy in spreads[j, k]:
                copy.wait_recv()
        for p in range(PIECES):
            load = merged(j, own, p)
            heads = [in_heads[j, k, p] for k in range(own)]
            gains = [head * (1.0 / GAIN) for head in heads]
            fraction = functools.reduce(jnp.add, heads, load(field_count))
            scale = None
            if j < nz - 1:
                scale = jnp.where(fraction > 0.0, GAIN / fraction, 0.0)
            for f in range(0, field_count, 2):
                first, second = load(f), load(f + 1)
                for k in range(own):
                    a, b = decode(in_codes, gains[k], (j, k, p), f)
                    first, second = first + a, second + b
                if scale is None:
                    sums[p, f * TILE : (f + 1) * TILE] = first
                    sums[p, (f + 1) * TILE : (f + 2) * TILE] = second
                else:
                    pair = jnp.concatenate([first * scale, second * scale], axis=0)
                    code = jnp.round(pair).astype(jnp.int32).astype(jnp.int16)
                    far_codes[j, p, f * TILE : (f + 2) * TILE] = code
            if scale is None:
                sums[p, field_count * TILE : (field_count + 1) * TILE] = fraction
            else:
                far_heads[j, p] = fraction
        if j < nz - 1:
            zj = along(j)
            slot = lax.rem(zj - z + nz, nz) - 1
            to = device(y, x, core, zj)
            send(far_codes.at[j], got_codes.at[slot], to, far_slots + 3 * slot)
            send(far_heads.at[j], got_heads.at[slot], to, far_slots + 3 * slot + 1)
        if j == 0:
            total = chip_tot[1]
            for k, copy in enumerate(near_copies):
                copy.wait_recv()
                total = total + near_tot[k]
            plane_tot[...] = total
            for k in range(1, nz):
                to = device(y, x, core, lax.rem(z + k, nz))
                send(plane_tot, far_tot.at[k - 1], to, far_slots + 3 * (k - 1) + 2)

    total = plane_tot[...]
    for k in range(nz - 1):
        for src, dst, which in (
            (far_codes.at[k], got_codes.at[k], 0),
            (far_heads.at[k], got_heads.at[k], 1),
            (plane_tot, far_tot.at[k], 2),
        ):
            pltpu.make_async_remote_copy(
                src_ref=src,
                dst_ref=dst,
                send_sem=send_sem.at[0],
                recv_sem=recv_sem.at[far_slots + 3 * k + which],
                device_id=device(y, x, core, lax.rem(z + k + 1, nz)),
                device_id_type=pl.DeviceIdType.MESH,
            ).wait_recv()
        total = total + far_tot[k]
    row, column = field_count % TILE, field_count // TILE
    means = total / jnp.maximum(total[row : row + 1, column : column + 1], 1.0)
    for p in range(PIECES):
        heads = [got_heads[k, p] for k in range(nz - 1)]
        gains = [head * (1.0 / GAIN) for head in heads]
        own_fraction = sums[p, field_count * TILE : (field_count + 1) * TILE]
        fraction = functools.reduce(jnp.add, heads, own_fraction)
        short = jnp.maximum(0.25 - fraction, 0.0)
        least = 1.0 / jnp.maximum(fraction, 0.25)
        for f in range(0, field_count, 2):
            tiles = [sums[p, (f + i) * TILE : (f + i + 1) * TILE] for i in range(2)]
            for k in range(nz - 1):
                tiles = [a + b for a, b in zip(tiles, decode(got_codes, gains[k], (k, p), f))]
            for i in range(2):
                row, column = (f + i) % TILE, (f + i) // TILE
                mean = means[row : row + 1, column : column + 1]
                start = (f + i) * TB_DEV + p * TILE
                result[start : start + TILE] = (tiles[i] + short * mean) * least
    for t in range(TB_DEV):
        columns = result[pl.ds(t, field_count, stride=TB_DEV), :]
        out_ref[:, t * cells : (t + 1) * cells] = columns
    for copy in started:
        copy.wait_send()


def body(sizes, fields, land_mask, intersection, send_slot, target_block, live_blocks):
    block_count, cells = intersection.shape[0], intersection.shape[1]
    field_count = fields.shape[0]
    nx, ny, nz = sizes["x"], sizes["y"], sizes["z"]
    owners = ny * nx * 2 * nz
    capacity = max(2, 2 * block_count // owners)
    stride = field_count + 1
    span = TB_DEV * stride
    steps = block_count // GROUP
    vmem = pl.BlockSpec(memory_space=pltpu.VMEM)
    acc, tot = pl.pallas_call(
        functools.partial(contribute, capacity, owners),
        in_specs=[pl.BlockSpec(memory_space=pl.ANY)] * 6,
        out_specs=[vmem, vmem],
        out_shape=[
            jax.ShapeDtypeStruct((owners * span + TILE, cells), jnp.float32),
            jax.ShapeDtypeStruct((TILE, cells), jnp.float32),
        ],
        scratch_shapes=[
            pltpu.VMEM((steps, field_count, GROUP * cells), jnp.bfloat16),
            pltpu.VMEM((steps, GROUP, cells), jnp.int32),
            pltpu.VMEM((steps, GROUP, cells, cells), jnp.bfloat16),
            pltpu.VMEM((16, GROUP * cells), jnp.float32),
            pltpu.VMEM((2, GROUP * 16, cells), jnp.float32),
            pltpu.VMEM((16, cells), jnp.float32),
            pltpu.SMEM(send_slot.shape, jnp.int32),
            pltpu.SMEM(target_block.shape, jnp.int32),
            pltpu.SMEM(live_blocks.shape, jnp.int32),
            pltpu.SemaphoreType.DMA((3, steps)),
            pltpu.SemaphoreType.DMA((3,)),
        ],
        compiler_params=pltpu.CompilerParams(
            vmem_limit_bytes=40 * 2**20
        ),
    )(
        in_hbm(send_slot),
        in_hbm(target_block),
        live_blocks,
        in_hbm(fields),
        in_hbm(land_mask.reshape(block_count, cells)),
        in_hbm(intersection),
    )

    plane = ny * nx
    code, head = (PIECES, field_count * TILE, cells), (PIECES, TILE, cells)
    near, far = (nz, plane - 1), (nz - 1,)
    copies = 1 + nz * plane + (plane - 1) * (2 * nz + 1) + 6 * (nz - 1)
    return pl.pallas_call(
        functools.partial(exchange, sizes, field_count),
        in_specs=[vmem, vmem],
        out_specs=vmem,
        out_shape=jax.ShapeDtypeStruct((field_count, TB_DEV * cells), jnp.float32),
        scratch_shapes=[
            pltpu.VMEM((nz, plane, span, cells), jnp.float32),
            pltpu.VMEM((*near, *code), jnp.int16),
            pltpu.VMEM((*near, *head), jnp.float32),
            pltpu.VMEM((*near, *code), jnp.int16),
            pltpu.VMEM((*near, *head), jnp.float32),
            pltpu.VMEM((*far, *code), jnp.int16),
            pltpu.VMEM((*far, *head), jnp.float32),
            pltpu.VMEM((*far, *code), jnp.int16),
            pltpu.VMEM((*far, *head), jnp.float32),
            pltpu.VMEM((PIECES, stride * TILE, cells), jnp.float32),
            pltpu.VMEM((field_count * TB_DEV, cells), jnp.float32),
            pltpu.VMEM((2, TILE, cells), jnp.float32),
            pltpu.VMEM((plane - 1, TILE, cells), jnp.float32),
            pltpu.VMEM((TILE, cells), jnp.float32),
            pltpu.VMEM((nz - 1, TILE, cells), jnp.float32),
            pltpu.SemaphoreType.DMA((copies,)),
            pltpu.SemaphoreType.DMA((copies,)),
        ],
        compiler_params=pltpu.CompilerParams(
            collective_id=0, has_side_effects=True, vmem_limit_bytes=50 * 2**20
        ),
    )(acc, tot)


def solution(mesh):
    band, sub = mesh.shape["band"], mesh.shape["sub"]
    plane = band // 2
    nx = max(d for d in range(1, math.isqrt(plane) + 1) if plane % d == 0)
    sizes = {"y": plane // nx, "x": nx, "z": sub}
    return jax.shard_map(
        functools.partial(body, sizes),
        mesh=mesh,
        in_specs=(
            P(None, ("band", "sub")),
            P(("band", "sub")),
            P(("band", "sub"), None, None),
            P(("band", "sub")),
            P(("band", "sub")),
            P(("band", "sub")),
        ),
        out_specs=P(None, ("band", "sub")),
        check_vma=False,
    )
```
